32 devices in a mesh: fsdp: 4 (over x, core), tensor: 4 (over z), dp: 2 (over y).
Axes of the slice: x: 2, y: 2, z: 4, core: 2. Of those that a mesh axis runs over, the one named last changes fastest.
Arguments:
- tokens: bfloat16 [1024, 8192], P('fsdp', 'dp'), may hold values from -6 to 6
- cotangent: bfloat16 [1024, 8192], P('fsdp', 'dp'), may hold values from -6 to 6
- gate_weight: bfloat16 [8192, 28672], P('fsdp', ('tensor', 'dp')), may hold values from -0.0625 to 0.0625
- up_weight: bfloat16 [8192, 28672], P('fsdp', ('tensor', 'dp')), may hold values from -0.0625 to 0.0625
- down_weight: bfloat16 [28672, 8192], P(('tensor', 'dp'), 'fsdp'), may hold values from -0.03125 to 0.03125
- model_projection: bfloat16 [64, 8192], replicated, may hold values from -0.0625 to 0.0625
- hidden_projection: bfloat16 [64, 28672], P(None, ('tensor', 'dp')), may hold values from -0.03125 to 0.03125
- queries: bfloat16 [256, 12288], P('dp'), may hold values from -0.0546875 to 0.0546875
Outputs:
- scores: float32 [256, 8], P('dp', 'fsdp')
The draws below stay inside these ranges and needn't reach their ends.
All inputs are finite; a program needn't handle non-finite values.
Results may differ from the reference program's by a relative error of at most 0.003.
Values may be sent and summed in bfloat16 or wider, within the bound.
No kernel may reach another device: no remote copies, remote signals or barrier semaphores. Data moves between devices by JAX's collectives and lax.ppermute only.
A program may use at most 320 MiB of HBM per device.

```python
import jax
import jax.numpy as jnp
from jax import lax

D = 8192
FF = 28672
RANK = 64
SEQ_LEN = 128
QUERIES = 256
TOKENS = 1024


def steps_of(key, shape, split, least, high):
    level, own = 1.0, jax.random.fold_in(key, 6)
    for position, blocks in split:
        steps = jnp.exp(jax.random.uniform(jax.random.fold_in(own, position), (blocks,), jnp.float32, least / len(split), high / len(split)))
        level = level * jnp.repeat(steps, shape[position] // blocks).reshape([-1 if axis == position else 1 for axis in range(len(shape))])
    return level


def noise(rng, shape, width, bound, pieces=(), dtype=jnp.bfloat16):
    factor_of = steps_of(rng, shape, pieces, -0.22, 0.18) if pieces else 1.0
    result = jax.random.normal(rng, shape, jnp.float32) * width * factor_of
    return jnp.minimum(jnp.maximum(result, -bound), bound).astype(dtype)


def setup_inputs(seed: int = 0) -> dict:
    splits = jax.random.split(jax.random.key(seed), 9)
    tokens = noise(splits[0], (TOKENS, D), 1.0, 6.0, ((0, 4), (1, 2)))
    cotangent = noise(splits[1], (TOKENS, D), 1.0, 6.0, ((0, 4), (1, 2)))
    gate_weight = noise(splits[2], (D, FF), D ** -0.5, 0.0625, ((0, 4), (1, 8)))
    up_weight = noise(splits[3], (D, FF), D ** -0.5, 0.0625, ((0, 4), (1, 8)))
    down_weight = noise(splits[4], (FF, D), FF ** -0.5, 0.03125, ((0, 8), (1, 4)))
    model_projection = noise(splits[5], (RANK, D), D ** -0.5, 0.0625)
    hidden_projection = noise(splits[6], (RANK, FF), FF ** -0.5, 0.03125, ((1, 8),))
    queries = noise(splits[7], (QUERIES, 3 * RANK * RANK), (3 * RANK * RANK) ** -0.5, 0.0546875, ((0, 2),))
    return dict(tokens=tokens, cotangent=cotangent, gate_weight=gate_weight, up_weight=up_weight, down_weight=down_weight, model_projection=model_projection, hidden_projection=hidden_projection, queries=queries)


def reference(tokens, cotangent, gate_weight, up_weight, down_weight, model_projection, hidden_projection, queries):
    gate_pre = jnp.dot(tokens, gate_weight, preferred_element_type=jnp.float32)
    up_pre = jnp.dot(tokens, up_weight, preferred_element_type=jnp.float32)
    sigmoid_gate = jax.nn.sigmoid(gate_pre)
    activated = gate_pre * sigmoid_gate
    hidden = (activated * up_pre).astype(jnp.bfloat16)
    back_grad = jnp.dot(cotangent, down_weight.T, preferred_element_type=jnp.float32)
    grad_gate = (back_grad * up_pre * sigmoid_gate * (1.0 + gate_pre * (1.0 - sigmoid_gate))).astype(jnp.bfloat16)
    grad_up = (back_grad * activated).astype(jnp.bfloat16)
    model_tok = jnp.dot(tokens, model_projection.T, preferred_element_type=jnp.float32)
    model_cot = jnp.dot(cotangent, model_projection.T, preferred_element_type=jnp.float32)
    proj_gate = jnp.dot(grad_gate, hidden_projection.T, preferred_element_type=jnp.float32)
    proj_up = jnp.dot(grad_up, hidden_projection.T, preferred_element_type=jnp.float32)
    proj_hidden = jnp.dot(hidden, hidden_projection.T, preferred_element_type=jnp.float32)
    seq_count = tokens.shape[0] // SEQ_LEN

    def shaped(matrix):
        return matrix.reshape(seq_count, SEQ_LEN, RANK)

    high = lax.Precision.HIGHEST
    g_gate = jnp.einsum("sti,stj->sij", shaped(model_tok), shaped(proj_gate), precision=high)
    g_up = jnp.einsum("sti,stj->sij", shaped(model_tok), shaped(proj_up), precision=high)
    g_down = jnp.einsum("sti,stj->sij", shaped(proj_hidden), shaped(model_cot), precision=high)
    grads = jnp.stack((g_gate, g_up, g_down), axis=1).reshape(seq_count, 3 * RANK * RANK)
    return jnp.dot(queries.astype(jnp.float32), grads.T, precision=high)
```

```python
import functools

import jax
import jax.numpy as jnp
from jax import lax
from jax.experimental import pallas as pl
from jax.experimental.pallas import tpu as pltpu
from jax.sharding import PartitionSpec as P


SEQ_LEN = 128
SEND_TOP = 32768.0
TILE = 256


def right_dot(left, right):
    return lax.dot_general(
        left, right, (((1,), (1,)), ((), ())), preferred_element_type=jnp.float32
    )


def left_dot(left, right):
    return jnp.dot(left, right, preferred_element_type=jnp.float32)


def swap(array, axis, size, bit):
    return lax.ppermute(array, axis, [(i, i ^ bit) for i in range(size)])


def butterfly(array, axis, size):
    bit = 1
    while bit < size:
        array = array + swap(array, axis, size, bit)
        bit *= 2
    return array


def part(array, index, count, axis):
    size = array.shape[axis] // count
    return lax.dynamic_slice_in_dim(array, index * size, size, axis)


def packed(partial):
    top = jnp.maximum(jnp.max(jnp.abs(partial), axis=1, keepdims=True), 1e-30)
    return (partial * (SEND_TOP / top)).astype(jnp.float16), top * (1.0 / SEND_TOP)


def product_kernel(contract, place, after, rows_kept, rows_came, kept, came, out, done):
    def dot(left, right):
        return lax.dot_general(
            left[...], right[...], (((1,), (contract,)), ((), ())), preferred_element_type=jnp.float32
        )

    out[...] = dot(rows_kept, kept) + dot(rows_came, came)
    done[...] = jnp.zeros_like(done)


def product(rows, core, weight, came, contract, after):
    width = came.shape[1 - contract]
    depth = came.shape[contract]
    count = rows.shape[0]
    if width % TILE:
        kept = part(weight, core, 2, 1 - contract)
        dot = right_dot if contract else left_dot
        out = dot(part(rows, core, 2, 1), kept) + dot(part(rows, 1 - core, 2, 1), came)
        return out, after
    steps = width // TILE
    block = (TILE, depth) if contract else (depth, TILE)

    def tile(index):
        return (index, 0) if contract else (0, index)

    return pl.pallas_call(
        functools.partial(product_kernel, contract),
        grid_spec=pltpu.PrefetchScalarGridSpec(
            num_scalar_prefetch=1,
            grid=(steps,),
            in_specs=[
                pl.BlockSpec(memory_space=pl.ANY),
                pl.BlockSpec((count, depth), lambda i, s: (0, s[0])),
                pl.BlockSpec((count, depth), lambda i, s: (0, 1 - s[0])),
                pl.BlockSpec(block, lambda i, s: tile(s[0] * steps + i)),
                pl.BlockSpec(block, lambda i, s: tile(i)),
            ],
            out_specs=[
                pl.BlockSpec((count, TILE), lambda i, s: (0, i)),
                pl.BlockSpec((8, 128), lambda i, s: (0, 0)),
            ],
        ),
        out_shape=[
            jax.ShapeDtypeStruct((count, width), jnp.float32),
            jax.ShapeDtypeStruct((8, 128), jnp.float32),
        ],
        compiler_params=pltpu.CompilerParams(dimension_semantics=("arbitrary",)),
        cost_estimate=pl.CostEstimate(
            flops=4 * count * depth * width,
            bytes_accessed=4 * depth * (width + count) + 4 * count * width,
            transcendentals=0,
        ),
    )(core.astype(jnp.int32).reshape(1), after, rows, rows, weight, came)


def on_device(
    sizes,
    tokens,
    cotangent,
    gate_weight,
    up_weight,
    down_weight,
    model_projection,
    hidden_projection,
    queries,
):
    fsdp, tensor, dp = sizes
    place = lax.axis_index("fsdp")
    side, core = place // 2, place % 2
    turn = lax.axis_index("tensor") % 2

    def sides(rows):
        if dp == 2:
            across = swap(rows, "dp", dp, 1)
            match = lax.axis_index("dp") == side
            return jnp.where(match, rows, across), jnp.where(match, across, rows)
        full = lax.all_gather(rows, "dp", axis=1, tiled=True)
        return part(full, side, 2, 1), part(full, 1 - side, 2, 1)

    first_tok, first_cot = part(tokens, turn, 2, 0), part(cotangent, turn, 2, 0)
    tok_mine, tok_theirs = sides(first_tok)
    tok_far = swap(tok_theirs, "fsdp", fsdp, 2)
    first_cot, tok_mine = lax.optimization_barrier((first_cot, tok_mine))
    cot_mine, cot_theirs = sides(first_cot)
    cot_far = swap(cot_theirs, "fsdp", fsdp, 2)
    tok_far_2 = swap(tok_far, "tensor", tensor, 1)
    tok_mine_2 = swap(tok_mine, "tensor", tensor, 1)
    cot_far_2 = swap(cot_far, "tensor", tensor, 1)
    cot_mine_2 = swap(cot_mine, "tensor", tensor, 1)

    gate_came = swap(part(gate_weight, 1 - core, 2, 1), "fsdp", fsdp, 1)
    up_came = swap(part(up_weight, 1 - core, 2, 1), "fsdp", fsdp, 1)
    down_came = swap(part(down_weight, 1 - core, 2, 0), "fsdp", fsdp, 1)

    def gathered(far, mine):
        pieces = (far, swap(far, "fsdp", fsdp, 1), mine, swap(mine, "fsdp", fsdp, 1))
        return jnp.concatenate(pieces, axis=0)

    def sent(partial):
        count = partial.shape[0] // 2
        values, scale = packed(partial[:count])
        return swap(values, "fsdp", fsdp, 2), scale

    def model(mine, theirs):
        return right_dot(mine, part(model_projection, side, 2, 1)) + right_dot(
            theirs, part(model_projection, 1 - side, 2, 1)
        )

    rank_size = model_projection.shape[0]
    half = tokens.shape[0] // 2
    seq_count = half // SEQ_LEN
    projection = part(hidden_projection, core, 2, 1)
    high = lax.Precision.HIGHEST

    def shaped(matrix):
        return matrix.reshape(seq_count, SEQ_LEN, rank_size)

    def scored(near, far, model_tok, model_cot):
        gate_pre, up_pre, back_grad = (
            mine[2 * half :] + values.astype(jnp.float32) * scale for mine, values, scale in zip(near, *far)
        )
        sigmoid_gate = jax.nn.sigmoid(gate_pre)
        activated = gate_pre * sigmoid_gate
        hidden = (activated * up_pre).astype(jnp.bfloat16)
        grad_gate = (
            back_grad * up_pre * sigmoid_gate * (1.0 + gate_pre * (1.0 - sigmoid_gate))
        ).astype(jnp.bfloat16)
        grad_up = (back_grad * activated).astype(jnp.bfloat16)
        stacked = jnp.concatenate(
            [m[:half] for m in (grad_gate, grad_up, hidden)] + [m[half:] for m in (grad_gate, grad_up, hidden)],
            axis=0,
        )
        projected = right_dot(stacked, projection)
        proj = projected[: 3 * half] + swap(projected[3 * half :], "fsdp", fsdp, 1)
        model_tok, model_cot = shaped(model_tok), shaped(model_cot)
        g_gate = jnp.einsum("sti,stj->sij", model_tok, shaped(proj[:half]), precision=high)
        g_up = jnp.einsum("sti,stj->sij", model_tok, shaped(proj[half : 2 * half]), precision=high)
        g_down = jnp.einsum("sti,stj->sij", shaped(proj[2 * half :]), model_cot, precision=high)
        grads = jnp.stack((g_gate, g_up, g_down), axis=1).reshape(seq_count, 3 * rank_size * rank_size)
        grads = butterfly(grads, "dp", dp)
        return jnp.dot(queries.astype(jnp.float32), grads.T, precision=high)

    def neighbour(rows):
        return swap(rows, "tensor", tensor, 1)

    def products(tok_rows, cot_rows, after):
        near, far, scales = [], [], []
        for rows, weight, came, contract in (
            (tok_rows, gate_weight, gate_came, 0),
            (tok_rows, up_weight, up_came, 0),
            (cot_rows, down_weight, down_came, 1),
        ):
            value, after = product(rows, core, weight, came, contract, after)
            values, scale = sent(value)
            near.append(value)
            far.append(values)
            scales.append(scale)
        scale = swap(jnp.concatenate(scales, axis=1), "fsdp", fsdp, 2)
        return near, (far, jnp.split(scale, 3, axis=1)), after

    after = jnp.zeros((8, 128), jnp.float32)
    near_1, far_1, after = products(gathered(tok_far, tok_mine), gathered(cot_far, cot_mine), after)
    near_2, far_2, after = products(gathered(tok_far_2, tok_mine_2), gathered(cot_far_2, cot_mine_2), after)
    near_1, near_2, _ = lax.optimization_barrier((near_1, near_2, after))

    model_tok_1, model_cot_1 = model(tok_mine, tok_theirs), model(cot_mine, cot_theirs)
    model_tok_2, model_cot_2 = neighbour(model_tok_1), neighbour(model_cot_1)
    first = scored(near_1, far_1, model_tok_1, model_cot_1)
    second = scored(near_2, far_2, model_tok_2, model_cot_2)
    scores = jnp.where(
        turn == 0, jnp.concatenate((first, second), axis=1), jnp.concatenate((second, first), axis=1)
    )
    return butterfly(scores, "tensor", tensor)


def solution(mesh):
    sizes = tuple(mesh.shape[name] for name in ("fsdp", "tensor", "dp"))
    assert sizes[0] == 4

    def body(*args):
        return on_device(sizes, *args)

    return jax.shard_map(
        body,
        mesh=mesh,
        in_specs=(
            P("fsdp", "dp"),
            P("fsdp", "dp"),
            P("fsdp", ("tensor", "dp")),
            P("fsdp", ("tensor", "dp")),
            P(("tensor", "dp"), "fsdp"),
            P(),
            P(None, ("tensor", "dp")),
            P("dp", None),
        ),
        out_specs=P("dp", "fsdp"),
        check_vma=False,
    )
```
